1024 devices in a mesh: gx: 8 (over x_lo, core), gy: 16 (over x_hi, z), gz: 8 (over y).
Axes of the slice: x: 8 (x_hi: 2, x_lo: 4; x = x_hi * 4 + x_lo), y: 8, z: 8, core: 2. Of those that a mesh axis runs over, the one named last changes fastest.
Arguments:
- encoded: bfloat16 [8, 1024, 4096], P('gx', None, 'gy'), may hold values from -6 to 6
- lengths: int32 [8], P('gx'), may hold values from 128 to 1024, as said below
- kv_weight: bfloat16 [4096, 64, 128], P('gy', 'gz'), may hold values from -0.09375 to 0.09375
Outputs:
- keys_values: bfloat16 [8, 1024, 64, 128], P('gx', 'gy', 'gz')
The draws below stay inside these ranges and needn't reach their ends.
Inputs may be any that keep to these rules, and one draw needn't show every extreme that they name: `lengths`: every length is a multiple of 128; some sequence has length 1024 and some has length 128.
All inputs are finite; a program needn't handle non-finite values.
Results may differ from the reference program's by a relative error of at most 0.001.
Values may be sent and summed in bfloat16 or wider, within the bound.
A program may use at most 32 MiB of HBM per device.

```python
import jax
import jax.numpy as jnp
from jax import lax

D = 4096
HEADS = 64
HEAD_DIM = 64
LMAX = 1024
SEQS = 8


def draw_lengths(key, part):
    tiles = jax.random.randint(key, (SEQS,), 1, LMAX // 128 + 1)
    tiles = tiles.at[0].set(LMAX // 128)
    tiles = tiles.at[SEQS - 1].set(1)
    return (tiles * 128).astype(jnp.int32)


def block_levels(rng, shape, pieces, smallest, high):
    def one(dim, shards_of):
        steps = jax.random.uniform(jax.random.fold_in(jax.random.fold_in(rng, 6), dim), (shards_of,), jnp.float32, smallest / len(pieces), high / len(pieces))
        return jnp.repeat(jnp.exp(steps), shape[dim] // shards_of).reshape((-1,) + (1,) * (len(shape) - dim - 1))

    factor_of = one(*pieces[0])
    for cut in pieces[1:]:
        factor_of = factor_of * one(*cut)
    return factor_of


def noise(own_key, dims, scale, bound, cuts=(), kind=jnp.bfloat16):
    gain = block_levels(own_key, dims, cuts, -0.22, 0.18) if cuts else 1.0
    entries = jax.random.normal(own_key, dims, jnp.float32) * scale * gain
    return jnp.minimum(jnp.maximum(entries, -bound), bound).astype(kind)


def setup_inputs(seed: int = 0) -> dict:
    splits = jax.random.split(jax.random.key(seed), 4)
    encoded = noise(splits[0], (SEQS, LMAX, D), 1.0, 6.0, ((0, 8), (2, 16)))
    lengths = draw_lengths(jax.random.fold_in(splits[3], 71), 0)
    kv_weight = noise(splits[2], (D, HEAD_DIM, 2 * HEADS), D ** -0.5, 0.09375, ((0, 16), (1, 8)))
    return {"encoded": encoded, "lengths": lengths, "kv_weight": kv_weight}


def reference(encoded, lengths, kv_weight):
    weight = kv_weight.reshape(D, HEAD_DIM, 2, HEADS)
    weight = jnp.transpose(weight, (0, 3, 2, 1)).reshape(D, HEADS * 2 * HEAD_DIM)
    places = jnp.arange(LMAX, dtype=jnp.int32)

    def project(item):
        states, length = item
        product = jnp.dot(states, weight, preferred_element_type=jnp.float32)
        kept = jnp.where((places < length)[:, None], product, jnp.zeros_like(product))
        return kept.astype(jnp.bfloat16).reshape(LMAX, HEADS, 2 * HEAD_DIM)

    return lax.map(project, (encoded, lengths))
```

```python
import jax
import jax.numpy as jnp
from jax import lax
from jax.experimental import pallas as pl
from jax.experimental.pallas import tpu as pltpu
from jax.sharding import Mesh
from jax.sharding import PartitionSpec as P

MESH = pl.DeviceIdType.MESH
RING = 8
BF16 = jnp.bfloat16
F32 = jnp.float32


def project(
    e_ref, len_ref, w_ref, out_ref,
    states, staged, weights, acc, perm, parts, arrived,
    far_send, far_recv, y_send, y_recv, z_send, z_recv, chip_send, chip_recv,
):
    xh, z, y, c = (lax.axis_index(a) for a in ("xh", "z", "y", "c"))
    other = 1 - xh
    mate = {"xh": other}
    twin = {"c": 1 - c}
    upper, quarter = y // 4, lax.rem(y, 4)

    def turn(base, by):
        return lax.rem(base + by + 2 * RING, RING)

    def remote(src, dst, send, recv, to):
        return pltpu.make_async_remote_copy(
            src_ref=src, dst_ref=dst, send_sem=send, recv_sem=recv, device_id=to, device_id_type=MESH
        )

    barrier = pltpu.get_barrier_semaphore()

    def greet(i, carry):
        pl.semaphore_signal(barrier, inc=1, device_id={"z": turn(z, i)}, device_id_type=MESH)
        pl.semaphore_signal(barrier, inc=1, device_id={"y": turn(y, i)}, device_id_type=MESH)
        return carry

    lax.fori_loop(1, RING, greet, 0)
    pl.semaphore_signal(barrier, inc=1, device_id=mate, device_id_type=MESH)
    pl.semaphore_signal(barrier, inc=1, device_id=twin, device_id_type=MESH)
    pl.semaphore_wait(barrier, 2 * (RING - 1) + 2)

    e_far = remote(e_ref.at[upper, :, quarter], staged, far_send.at[0], far_recv.at[0], mate)
    e_far.start()
    w_far = remote(
        w_ref.at[pl.ds(c * 128, 128), pl.ds(pl.multiple_of(other * 512, 512), 512)],
        weights.at[z, xh, c], far_send.at[1], far_recv.at[1], mate,
    )
    w_far.start()
    w_far_in = remote(
        weights.at[z, other, c], weights.at[z, other, c], far_send.at[1], far_recv.at[1], mate
    )

    def spread(i, carry):
        to = turn(z, i)
        remote(
            e_ref.at[upper, to, quarter], states.at[y, xh, z], far_send.at[2], far_recv.at[2], {"z": to}
        ).start()
        return carry

    def spread_far(i, carry):
        to = turn(z, i)
        remote(
            staged.at[to], states.at[y, other, z], far_send.at[3], far_recv.at[3], {"z": to}
        ).start()
        return carry

    def seven(block, k):
        some = states.at[y, block, pl.ds(0, RING - 1)]
        return remote(some, some, far_send.at[k], far_recv.at[k], {"z": z})

    lax.fori_loop(1, RING, spread, 0)

    way = 1 - 2 * c
    ahead = {"z": turn(z, way)}

    def w_slot(phase, hop, short):
        source = turn(z, -way * hop)
        half = 1 - c if short else c
        return weights.at[source, xh if phase == 0 else other, half]

    def w_index(phase, hop, short):
        return phase * 7 + (hop - 1) * 2 + short

    def w_send(phase, hop, short, src):
        k = w_index(phase, hop + 1, short)
        remote(src, w_slot(phase, hop, short), z_send.at[k], z_recv.at[k], ahead).start()

    def w_take(phase, hop, short):
        k = w_index(phase, hop, short)
        slot = w_slot(phase, hop, short)
        remote(slot, slot, z_send.at[k], z_recv.at[k], ahead).wait_recv()
        if hop < 3 or (hop == 3 and not short):
            w_send(phase, hop, short, slot)
        remote(slot, slot, chip_send.at[k], chip_recv.at[k], twin).start()

    def own_weight(half):
        return w_ref.at[pl.ds(half * 128, 128), pl.ds(pl.multiple_of(xh * 512, 512), 512)]

    for short in (0, 1):
        w_send(0, 0, short, own_weight(1 - c if short else c))

    def y_slot(block, side, hop):
        source = turn(y, -hop if side == 0 else hop)
        return states.at[source, xh if block == 0 else other]

    def y_index(block, side, hop):
        return (block * 2 + side) * 4 + hop - 1

    def y_send_on(block, side, hop):
        k = y_index(block, side, hop + 1)
        slot = y_slot(block, side, hop)
        to = {"y": turn(y, 1 if side == 0 else -1)}
        remote(slot, slot, y_send.at[k], y_recv.at[k], to).start()

    def y_hops(block, side):
        return 4 if block == side else 3

    def y_take(block, side, hop):
        k = y_index(block, side, hop)
        slot = y_slot(block, side, hop)
        to = {"y": turn(y, 1 if side == 0 else -1)}
        remote(slot, slot, y_send.at[k], y_recv.at[k], to).wait_recv()
        if hop < y_hops(block, side):
            y_send_on(block, side, hop)

    states[y, xh, z] = e_ref[upper, z, quarter]
    for half in (0, 1):
        weights[z, xh, half] = w_ref[pl.ds(half * 128, 128), pl.ds(pl.multiple_of(xh * 512, 512), 512)]
    acc[...] = jnp.zeros_like(acc)

    def build(i, carry):
        column = lax.broadcasted_iota(jnp.int32, (1, 1024), 1)
        lane = lax.rem(column, 128)
        wanted = (
            (lane // 64) * 512
            + (lax.rem(lane, 64) // 16) * 128
            + (lax.rem(lane, 16) // 8) * 64
            + (column // 128) * 8
            + lax.rem(lane, 8)
        )
        row = lax.broadcasted_iota(jnp.int32, (64, 1024), 0) + i * 64
        perm[pl.ds(pl.multiple_of(i * 64, 64), 64), :] = jnp.where(row == wanted, 1.0, 0.0).astype(BF16)
        return carry

    lax.fori_loop(0, 16, build, 0)

    def multiply(block):
        side = xh if block == 0 else other

        def step(i, carry):
            left = states[:, side, i].reshape(128, 256)
            right = weights[i, side].reshape(256, 512)
            acc[...] += jnp.dot(left, right, preferred_element_type=F32)
            return carry

        lax.fori_loop(0, RING, step, 0)

    def chip_wait(phase):
        for k in range(phase * 7, phase * 7 + 7):
            hop, short = (k - phase * 7) // 2 + 1, (k - phase * 7) % 2
            source = turn(z, way * hop)
            half = c if short else 1 - c
            slot = weights.at[source, xh if phase == 0 else other, half]
            remote(slot, slot, chip_send.at[k], chip_recv.at[k], twin).wait_recv()

    seven(xh, 2).wait_recv()
    for side in (0, 1):
        y_send_on(0, side, 0)
    w_take(0, 1, 0)
    w_take(0, 1, 1)
    e_far.wait_recv()
    lax.fori_loop(1, RING, spread_far, 0)
    states[y, other, z] = staged[z]
    w_take(0, 2, 0)
    for side in (0, 1):
        y_take(0, side, 1)
    w_take(0, 2, 1)
    w_take(0, 3, 0)
    for side in (0, 1):
        y_take(0, side, 2)
    w_take(0, 3, 1)
    w_far_in.wait_recv()
    remote(
        weights.at[z, other, c], weights.at[z, other, c], chip_send.at[14], chip_recv.at[14], twin
    ).start()
    w_send(1, 0, 0, weights.at[z, other, c])
    seven(other, 3).wait_recv()
    for side in (0, 1):
        y_send_on(1, side, 0)
    theirs = weights.at[z, other, 1 - c]
    remote(theirs, theirs, chip_send.at[14], chip_recv.at[14], twin).wait_recv()
    w_send(1, 0, 1, theirs)
    w_take(0, 4, 0)
    for side in (0, 1):
        y_take(0, side, 3)
    for side in (0, 1):
        y_take(1, side, 1)
    w_take(1, 1, 0)
    w_take(1, 1, 1)
    y_take(0, 0, 4)
    for side in (0, 1):
        y_take(1, side, 2)
    w_take(1, 2, 0)
    w_take(1, 2, 1)
    chip_wait(0)
    multiply(0)
    for side in (0, 1):
        y_take(1, side, 3)
    w_take(1, 3, 0)
    w_take(1, 3, 1)
    y_take(1, 1, 4)
    w_take(1, 4, 0)
    chip_wait(1)
    multiply(1)

    row = lax.broadcasted_iota(jnp.int32, (128, 512), 0)
    place = (row // 64) * 512 + z * 64 + lax.rem(row, 64)
    total = acc[...]
    kept = jnp.where(place < len_ref[0], total, jnp.zeros_like(total)).astype(BF16).reshape(2, 2, 32, 512)
    sorted_parts = jnp.dot(
        kept[:, 0].reshape(64, 512), perm[pl.ds(0, 512), :], preferred_element_type=F32
    ) + jnp.dot(kept[:, 1].reshape(64, 512), perm[pl.ds(512, 512), :], preferred_element_type=F32)
    sorted_parts = sorted_parts.astype(BF16)
    for b in (0, 1):
        for j in range(RING):
            parts[b * RING + j] = sorted_parts[b * 32 : b * 32 + 32, j * 128 : j * 128 + 128]

    e_far.wait_send()
    w_far.wait_send()
    seven(xh, 2).wait_send()
    seven(other, 3).wait_send()
    for phase in (0, 1):
        for k in range(7):
            slot = w_slot(phase, k // 2 + 1, k % 2)
            k = phase * 7 + k
            remote(slot, slot, z_send.at[k], z_recv.at[k], ahead).wait_send()
            remote(slot, slot, chip_send.at[k], chip_recv.at[k], twin).wait_send()
    remote(theirs, theirs, chip_send.at[14], chip_recv.at[14], twin).wait_send()
    for block in (0, 1):
        for side in (0, 1):
            for hop in range(1, y_hops(block, side) + 1):
                k = y_index(block, side, hop)
                slot = y_slot(block, side, hop)
                remote(slot, slot, y_send.at[k], y_recv.at[k], {"y": y}).wait_send()

    me = xh * RING + y

    def deliver(i, carry):
        to = lax.rem(me + i, 2 * RING)
        remote(
            parts.at[to], arrived.at[me], far_send.at[4], far_recv.at[4],
            {"xh": to // RING, "y": lax.rem(to, RING)},
        ).start()
        return carry

    lax.fori_loop(1, 2 * RING, deliver, 0)
    arrived[me] = parts[me]
    most = arrived.at[pl.ds(0, 2 * RING - 1)]
    last = remote(most, most, far_send.at[4], far_recv.at[4], mate)
    last.wait_recv()
    out_ref[...] = arrived[...]
    last.wait_send()


def local(encoded, lengths, kv_weight):
    states = encoded.reshape(2, 8, 4, 16, 256)
    weight = kv_weight.reshape(256, 1024)
    vmem = pl.BlockSpec(memory_space=pltpu.VMEM)
    arrived = pl.pallas_call(
        project,
        out_shape=jax.ShapeDtypeStruct((16, 32, 128), BF16),
        in_specs=[vmem, pl.BlockSpec(memory_space=pltpu.SMEM), vmem],
        out_specs=vmem,
        scratch_shapes=[
            pltpu.VMEM((8, 2, 8, 16, 256), BF16),
            pltpu.VMEM((8, 16, 256), BF16),
            pltpu.VMEM((8, 2, 2, 128, 512), BF16),
            pltpu.VMEM((128, 512), F32),
            pltpu.VMEM((1024, 1024), BF16),
            pltpu.VMEM((16, 32, 128), BF16),
            pltpu.VMEM((16, 32, 128), BF16),
            pltpu.SemaphoreType.DMA((5,)),
            pltpu.SemaphoreType.DMA((5,)),
            pltpu.SemaphoreType.DMA((16,)),
            pltpu.SemaphoreType.DMA((16,)),
            pltpu.SemaphoreType.DMA((14,)),
            pltpu.SemaphoreType.DMA((14,)),
            pltpu.SemaphoreType.DMA((15,)),
            pltpu.SemaphoreType.DMA((15,)),
        ],
        compiler_params=pltpu.CompilerParams(collective_id=0, has_side_effects=True),
        name="project",
    )(states, lengths, weight)
    arrived = arrived.reshape(2, 8, 32, 2, 4, 2, 8)
    return jnp.transpose(arrived, (3, 2, 6, 5, 1, 0, 4)).reshape(1, 64, 8, 128)


def solution(mesh):
    torus = Mesh(mesh.devices.reshape(4, 2, 2, 8, 8), ("xl", "c", "xh", "z", "y"))
    placed = (P(("xl", "c"), None, ("xh", "z")), P(("xl", "c")), P(("xh", "z"), "y", None))
    return jax.shard_map(
        local, mesh=torus, in_specs=placed, out_specs=P(("xl", "c"), ("xh", "z"), "y", None), check_vma=False
    )
```

```python
import jax
import jax.numpy as jnp
from jax import lax
from jax.experimental import pallas as pl
from jax.experimental.pallas import tpu as pltpu
from jax.sharding import Mesh
from jax.sharding import PartitionSpec as P

MESH = pl.DeviceIdType.MESH
RING = 8
BF16 = jnp.bfloat16
F32 = jnp.float32


def project(
    e_in, len_ref, w_in, out_ref,
    e_ref, w_raw, w_ref, states, staged, weights, acc, perm, final, parts, arrived,
    load, far_send, far_recv, e_send, e_recv, y_send, y_recv, z_send, z_recv, chip_send, chip_recv,
):
    xh, z, y, c = (lax.axis_index(a) for a in ("xh", "z", "y", "c"))
    other = 1 - xh
    mate = {"xh": other}
    twin = {"c": 1 - c}
    upper, quarter = y // 4, lax.rem(y, 4)

    def turn(base, by):
        return lax.rem(base + by + 2 * RING, RING)

    def remote(src, dst, send, recv, to):
        return pltpu.make_async_remote_copy(
            src_ref=src, dst_ref=dst, send_sem=send, recv_sem=recv, device_id=to, device_id_type=MESH
        )

    def signal(sem, to):
        pl.semaphore_signal(sem, inc=1, device_id=to, device_id_type=MESH)

    barrier = pltpu.get_barrier_semaphore()

    def greet(i, carry):
        signal(barrier, {"z": turn(z, i)})
        return carry

    lax.fori_loop(1, RING, greet, 0)
    for dy in (1, -1, 2, -2):
        signal(barrier, {"y": turn(y, dy)})
    signal(barrier, mate)
    signal(barrier, twin)
    w_load = pltpu.make_async_copy(w_in, w_raw, load.at[0])
    w_load.start()
    e_load = pltpu.make_async_copy(e_in, e_ref, load.at[1])
    e_load.start()
    w_load.wait()
    for e in range(8):
        w_ref[:, e * 128 : e * 128 + 128] = w_raw[:, e, :]
    e_load.wait()
    pl.semaphore_wait(barrier, RING - 1 + 6)

    def far_weights(sub):
        return remote(
            w_ref.at[pl.ds(c * 128 + sub * 64, 64), pl.ds(pl.multiple_of(other * 512, 512), 512)],
            weights.at[z, xh, c * 2 + sub], far_send.at[1 + sub], far_recv.at[1 + sub], mate,
        )

    w_far = [far_weights(sub) for sub in (0, 1)]
    for sub in (0, 1):
        w_far[sub].start()
    e_far = remote(e_ref.at[upper, :, quarter], staged, far_send.at[0], far_recv.at[0], mate)
    e_far.start()

    way = 1 - 2 * c
    next_z = turn(z, way)
    ahead = {"z": next_z}

    def w_slot(phase, hop, short, sub):
        source = turn(z, -way * hop)
        half = 1 - c if short else c
        return weights.at[source, xh if phase == 0 else other, half * 2 + sub]

    def w_index(phase, hop, short, sub):
        return phase * 14 + (hop - 1) * 4 + short * 2 + sub

    def w_send(phase, hop, short, sub, src):
        k = w_index(phase, hop + 1, short, sub)
        remote(src, w_slot(phase, hop, short, sub), z_send.at[k], z_recv.at[k], ahead).start()

    def w_take(phase, hop, short):
        for sub in (0, 1):
            k = w_index(phase, hop, short, sub)
            slot = w_slot(phase, hop, short, sub)
            remote(slot, slot, z_send.at[k], z_recv.at[k], ahead).wait_recv()
            if hop < 3 or (hop == 3 and not short):
                w_send(phase, hop, short, sub, slot)
            remote(slot, slot, chip_send.at[k], chip_recv.at[k], twin).start()

    def own_weight(short):
        half = 1 - c if short else c
        for sub in (0, 1):
            w_send(
                0, 0, short, sub,
                w_ref.at[pl.ds(half * 128 + sub * 64, 64), pl.ds(pl.multiple_of(xh * 512, 512), 512)],
            )

    def far_own():
        for sub in (0, 1):
            slot = weights.at[z, other, c * 2 + sub]
            remote(slot, slot, far_send.at[1 + sub], far_recv.at[1 + sub], mate).wait_recv()
            w_send(1, 0, 0, sub, slot)
            remote(slot, slot, chip_send.at[28 + sub], chip_recv.at[28 + sub], twin).start()

    def twin_own():
        for sub in (0, 1):
            slot = weights.at[z, other, (1 - c) * 2 + sub]
            remote(slot, slot, chip_send.at[28 + sub], chip_recv.at[28 + sub], twin).wait_recv()
            w_send(1, 0, 1, sub, slot)

    own_weight(0)

    def spread(to, carry):
        @pl.when(to != z)
        def _():
            remote(
                e_ref.at[upper, to, quarter], states.at[y, xh, z], e_send.at[to], e_recv.at[z], {"z": to}
            ).start()

        return carry

    def spread_far(to, carry):
        @pl.when(to != z)
        def _():
            remote(
                staged.at[to], states.at[y, other, z], e_send.at[RING + to], e_recv.at[RING + z], {"z": to}
            ).start()

        return carry

    def take_states(block, first, end):
        def one(source, carry):
            @pl.when(source != z)
            def _():
                slot = states.at[y, xh if block == 0 else other, source]
                k = block * RING + source
                remote(slot, slot, e_send.at[k], e_recv.at[k], {"z": z}).wait_recv()

            return carry

        lax.fori_loop(first, end, one, 0)

    lax.fori_loop(0, RING, spread, 0)
    own_weight(1)

    def far_states():
        e_far.wait_recv()
        lax.fori_loop(0, RING, spread_far, 0)
        states[y, other, z] = staged[z]

    REACH = ((4, 3), (3, 4))

    def y_index(block, side, distance):
        return (block * 2 + side) * 4 + distance - 1

    def y_copy(block, side, origin, distance):
        sign = 1 if side == 0 else -1
        slot = states.at[turn(y, -sign * origin), xh if block == 0 else other]
        k = y_index(block, side, distance)
        return remote(slot, slot, y_send.at[k], y_recv.at[k], {"y": turn(y, sign * (distance - origin))})

    def y_own(block):
        for distance in (2, 1):
            for side in (0, 1):
                y_copy(block, side, 0, distance).start()

    def y_relay(block):
        for side in (block, 1 - block):
            y_copy(block, side, 2, 2).wait_recv()
            for distance in range(REACH[block][side], 2, -1):
                y_copy(block, side, 2, distance).start()

    def y_rest(block):
        for distance in (1, 3, 4):
            for side in (0, 1):
                if distance <= REACH[block][side]:
                    y_copy(block, side, distance, distance).wait_recv()

    states[y, xh, z] = e_ref[upper, z, quarter]
    for q in range(4):
        weights[z, xh, q] = w_ref[q * 64 : q * 64 + 64, pl.ds(pl.multiple_of(xh * 512, 512), 512)]
    acc[...] = jnp.zeros_like(acc)

    column = lax.broadcasted_iota(jnp.int32, (1, 1024), 1)
    lane = lax.rem(column, 128)
    by_owner = (
        (lane // 64) * 512
        + (lax.rem(lane, 64) // 16) * 128
        + (lax.rem(lane, 16) // 8) * 64
        + (column // 128) * 8
        + lax.rem(lane, 8)
    )
    by_head = (
        (lax.rem(lane, 64) // 8) * 128
        + (lax.rem(lane, 8) // 4) * 64
        + lax.rem(lane, 4) * 16
        + (lane // 64) * 8
        + column // 128
    )

    def build(i, carry):
        row = lax.broadcasted_iota(jnp.int32, (64, 1024), 0) + i * 64
        here = pl.ds(pl.multiple_of(i * 64, 64), 64)
        perm[here, :] = jnp.where(row == by_owner, 1.0, 0.0).astype(BF16)
        final[here, :] = jnp.where(row == by_head, 1.0, 0.0).astype(BF16)
        return carry

    lax.fori_loop(0, 16, build, 0)

    def multiply(block, distances):
        side = xh if block == 0 else other
        total = acc[...]
        for d in distances:
            i = turn(z, d)
            total = total + jnp.dot(
                states[:, side, i].reshape(128, 256), weights[i, side].reshape(256, 512),
                preferred_element_type=F32,
            )
        acc[...] = total

    def chip_take(phase, hops):
        for hop in hops:
            for short in (0, 1):
                for sub in (0, 1):
                    if hop < 4 or not short:
                        k = w_index(phase, hop, short, sub)
                        half = c if short else 1 - c
                        slot = weights.at[turn(z, way * hop), xh if phase == 0 else other, half * 2 + sub]
                        remote(slot, slot, chip_send.at[k], chip_recv.at[k], twin).wait_recv()

    w_take(0, 1, 0)
    w_take(0, 1, 1)
    take_states(0, 0, RING)
    y_own(0)
    w_take(0, 2, 0)
    w_take(0, 2, 1)
    far_own()
    w_take(0, 3, 0)
    twin_own()
    w_take(0, 3, 1)
    y_relay(0)
    far_states()
    w_take(0, 4, 0)
    w_take(1, 1, 0)
    take_states(1, 0, RING)
    y_own(1)
    w_take(1, 1, 1)
    w_take(1, 2, 0)
    w_take(1, 2, 1)
    w_take(1, 3, 0)
    y_relay(1)
    w_take(1, 3, 1)
    chip_take(0, (1, 2, 3, 4))
    y_rest(0)
    multiply(0, range(8))
    w_take(1, 4, 0)
    y_rest(1)
    chip_take(1, (1, 2))
    multiply(1, (0, 1, 2, 6, 7))
    chip_take(1, (3, 4))
    multiply(1, (3, 4, 5))

    row = lax.broadcasted_iota(jnp.int32, (128, 512), 0)
    place = (row // 64) * 512 + z * 64 + lax.rem(row, 64)
    total = acc[...]
    kept = jnp.where(place < len_ref[0], total, jnp.zeros_like(total)).astype(BF16).reshape(2, 2, 32, 512)
    sorted_parts = jnp.dot(
        kept[:, 0].reshape(64, 512), perm[pl.ds(0, 512), :], preferred_element_type=F32
    ) + jnp.dot(kept[:, 1].reshape(64, 512), perm[pl.ds(512, 512), :], preferred_element_type=F32)
    sorted_parts = sorted_parts.astype(BF16)
    for b in (0, 1):
        for j in range(RING):
            parts[b * RING + j] = sorted_parts[b * 32 : b * 32 + 32, j * 128 : j * 128 + 128]

    e_far.wait_send()
    for sub in (0, 1):
        w_far[sub].wait_send()

    def sent(to, carry):
        @pl.when(to != z)
        def _():
            for k in (to, RING + to):
                slot = states.at[y, xh, z]
                remote(slot, slot, e_send.at[k], e_recv.at[k], {"z": z}).wait_send()

        return carry

    lax.fori_loop(0, RING, sent, 0)
    for phase in (0, 1):
        for k in range(phase * 14, phase * 14 + 14):
            slot = weights.at[z, xh, 0]
            remote(slot, slot, z_send.at[k], z_recv.at[k], ahead).wait_send()
            remote(slot, slot, chip_send.at[k], chip_recv.at[k], twin).wait_send()
    for k in (28, 29):
        slot = weights.at[z, xh, 0]
        remote(slot, slot, chip_send.at[k], chip_recv.at[k], twin).wait_send()
    for block in (0, 1):
        for side in (0, 1):
            for distance in range(1, REACH[block][side] + 1):
                y_copy(block, side, 0, distance).wait_send()

    me = xh * RING + y

    for across in (1, 0):
        for dy in (4, 3, 5, 2, 6, 1, 7, 0):
            if across or dy:
                to_xh, to_y = (other if across else xh), turn(y, dy)
                remote(
                    parts.at[to_xh * RING + to_y], arrived.at[me], far_send.at[3], far_recv.at[3],
                    {"xh": to_xh, "y": to_y},
                ).start()
    arrived[me] = parts[me]
    most = arrived.at[pl.ds(0, 2 * RING - 1)]
    last = remote(most, most, far_send.at[3], far_recv.at[3], mate)
    last.wait_recv()
    rows = [
        jnp.concatenate(
            [arrived[s * RING + j][:, p * 64 : p * 64 + 64] for j in range(RING) for s in (0, 1)], axis=1
        )
        for p in (0, 1)
    ]
    out_ref[...] = jnp.dot(jnp.concatenate(rows, axis=0), final[...], preferred_element_type=F32).astype(BF16)
    last.wait_send()


def local(encoded, lengths, kv_weight):
    states = encoded.reshape(2, 8, 4, 16, 256)
    vmem = pl.BlockSpec(memory_space=pltpu.VMEM)
    hbm = pl.BlockSpec(memory_space=pltpu.HBM)
    keys_values = pl.pallas_call(
        project,
        out_shape=jax.ShapeDtypeStruct((64, 1024), BF16),
        in_specs=[hbm, pl.BlockSpec(memory_space=pltpu.SMEM), hbm],
        out_specs=vmem,
        scratch_shapes=[
            pltpu.VMEM((2, 8, 4, 16, 256), BF16),
            pltpu.VMEM((256, 8, 128), BF16),
            pltpu.VMEM((256, 1024), BF16),
            pltpu.VMEM((8, 2, 8, 16, 256), BF16),
            pltpu.VMEM((8, 16, 256), BF16),
            pltpu.VMEM((8, 2, 4, 64, 512), BF16),
            pltpu.VMEM((128, 512), F32),
            pltpu.VMEM((1024, 1024), BF16),
            pltpu.VMEM((1024, 1024), BF16),
            pltpu.VMEM((16, 32, 128), BF16),
            pltpu.VMEM((16, 32, 128), BF16),
            pltpu.SemaphoreType.DMA((2,)),
            pltpu.SemaphoreType.DMA((4,)),
            pltpu.SemaphoreType.DMA((4,)),
            pltpu.SemaphoreType.DMA((16,)),
            pltpu.SemaphoreType.DMA((16,)),
            pltpu.SemaphoreType.DMA((16,)),
            pltpu.SemaphoreType.DMA((16,)),
            pltpu.SemaphoreType.DMA((28,)),
            pltpu.SemaphoreType.DMA((28,)),
            pltpu.SemaphoreType.DMA((30,)),
            pltpu.SemaphoreType.DMA((30,)),
        ],
        compiler_params=pltpu.CompilerParams(collective_id=0, has_side_effects=True),
        name="project",
    )(states, lengths, kv_weight)
    return keys_values.reshape(1, 64, 8, 128)


def solution(mesh):
    torus = Mesh(mesh.devices.reshape(4, 2, 2, 8, 8), ("xl", "c", "xh", "z", "y"))
    placed = (P(("xl", "c"), None, ("xh", "z")), P(("xl", "c")), P(("xh", "z"), "y", None))
    return jax.shard_map(
        local, mesh=torus, in_specs=placed, out_specs=P(("xl", "c"), ("xh", "z"), "y", None), check_vma=False
    )
```

```python
import jax
import jax.numpy as jnp
from jax import lax
from jax.experimental import pallas as pl
from jax.experimental.pallas import tpu as pltpu
from jax.sharding import Mesh
from jax.sharding import PartitionSpec as P

MESH = pl.DeviceIdType.MESH
RING = 8
BF16 = jnp.bfloat16
F32 = jnp.float32


def project(
    e_in, len_in, w_in, out_ref,
    len_ref, e_ref, w_raw, w_ref, states, weights, acc, perm, final, parts, arrived,
    load, far_send, far_recv, e_send, e_recv, y_send, y_recv, z_send, z_recv, chip_send, chip_recv,
):
    xh, z, y, c = (lax.axis_index(a) for a in ("xh", "z", "y", "c"))
    other = 1 - xh
    mate = {"xh": other}
    twin = {"c": 1 - c}
    upper, quarter = y // 4, lax.rem(y, 4)

    def turn(base, by):
        return lax.rem(base + by + 2 * RING, RING)

    def remote(src, dst, send, recv, to):
        return pltpu.make_async_remote_copy(
            src_ref=src, dst_ref=dst, send_sem=send, recv_sem=recv, device_id=to, device_id_type=MESH
        )

    def signal(sem, to):
        pl.semaphore_signal(sem, inc=1, device_id=to, device_id_type=MESH)

    def rows_of(q):
        half = c if q < 2 else 1 - c
        return pl.ds(pl.multiple_of(half * 128 + (q % 2) * 64, 64), 64)

    w_load = [pltpu.make_async_copy(w_in.at[rows_of(q)], w_raw.at[rows_of(q)], load.at[q]) for q in range(4)]
    e_load = pltpu.make_async_copy(e_in, e_ref, load.at[4])
    len_load = pltpu.make_async_copy(len_in, len_ref, load.at[5])
    w_load[0].start()
    w_load[1].start()
    e_load.start()
    w_load[2].start()
    w_load[3].start()
    len_load.start()

    barrier = pltpu.get_barrier_semaphore()

    def greet(i, carry):
        signal(barrier, {"z": turn(z, i)})
        return carry

    lax.fori_loop(1, RING, greet, 0)
    for dy in (1, -1, 2, -2):
        signal(barrier, {"y": turn(y, dy)})
    signal(barrier, mate)
    signal(barrier, twin)

    def lay_out(q):
        w_load[q].wait()
        for e in range(8):
            w_ref[rows_of(q), e * 128 : e * 128 + 128] = w_raw[rows_of(q), e, :]

    lay_out(0)
    lay_out(1)
    pl.semaphore_wait(barrier, RING - 1 + 6)

    def far_weights(sub):
        return remote(
            w_ref.at[pl.ds(c * 128 + sub * 64, 64), pl.ds(pl.multiple_of(other * 512, 512), 512)],
            weights.at[z, xh, c * 2 + sub], far_send.at[1 + sub], far_recv.at[1 + sub], mate,
        )

    w_far = [far_weights(sub) for sub in (0, 1)]
    e_far = remote(states.at[y, xh], states.at[y, xh], far_send.at[0], far_recv.at[0], mate)
    e_far_in = remote(states.at[y, other], states.at[y, other], far_send.at[0], far_recv.at[0], mate)
    w_far[0].start()
    w_far[1].start()

    way = 1 - 2 * c
    next_z = turn(z, way)
    ahead = {"z": next_z}

    def w_slot(phase, hop, short, sub):
        source = turn(z, -way * hop)
        half = 1 - c if short else c
        return weights.at[source, xh if phase == 0 else other, half * 2 + sub]

    def w_index(phase, hop, short, sub):
        return phase * 14 + (hop - 1) * 4 + short * 2 + sub

    def w_send(phase, hop, short, sub, src):
        k = w_index(phase, hop + 1, short, sub)
        remote(src, w_slot(phase, hop, short, sub), z_send.at[k], z_recv.at[k], ahead).start()

    def w_take(phase, hop, short):
        for sub in (0, 1):
            k = w_index(phase, hop, short, sub)
            slot = w_slot(phase, hop, short, sub)
            remote(slot, slot, z_send.at[k], z_recv.at[k], ahead).wait_recv()
            if hop < 3 or (hop == 3 and not short):
                w_send(phase, hop, short, sub, slot)
            remote(slot, slot, chip_send.at[k], chip_recv.at[k], twin).start()

    def own_weight(short):
        half = 1 - c if short else c
        for sub in (0, 1):
            w_send(
                0, 0, short, sub,
                w_ref.at[pl.ds(half * 128 + sub * 64, 64), pl.ds(pl.multiple_of(xh * 512, 512), 512)],
            )

    def far_own(sub):
        slot = weights.at[z, other, c * 2 + sub]
        remote(slot, slot, far_send.at[1 + sub], far_recv.at[1 + sub], mate).wait_recv()
        w_send(1, 0, 0, sub, slot)
        remote(slot, slot, chip_send.at[28 + sub], chip_recv.at[28 + sub], twin).start()

    def twin_own():
        for sub in (0, 1):
            slot = weights.at[z, other, (1 - c) * 2 + sub]
            remote(slot, slot, chip_send.at[28 + sub], chip_recv.at[28 + sub], twin).wait_recv()
            w_send(1, 0, 1, sub, slot)

    own_weight(0)
    e_load.wait()

    def spread(to, carry):
        @pl.when(to != z)
        def _():
            remote(
                e_ref.at[upper, to, quarter], states.at[y, xh, z], e_send.at[to], e_recv.at[z], {"z": to}
            ).start()

        return carry

    def take_states():
        def one(source, carry):
            @pl.when(source != z)
            def _():
                slot = states.at[y, xh, source]
                remote(slot, slot, e_send.at[source], e_recv.at[source], {"z": z}).wait_recv()

            return carry

        lax.fori_loop(0, RING, one, 0)

    lax.fori_loop(0, RING, spread, 0)
    lay_out(2)
    lay_out(3)
    own_weight(1)

    REACH = ((4, 3), (3, 4))

    def y_index(block, side, distance):
        return (block * 2 + side) * 4 + distance - 1

    def y_copy(block, side, origin, distance):
        sign = 1 if side == 0 else -1
        slot = states.at[turn(y, -sign * origin), xh if block == 0 else other]
        k = y_index(block, side, distance)
        return remote(slot, slot, y_send.at[k], y_recv.at[k], {"y": turn(y, sign * (distance - origin))})

    def y_own(block):
        for distance in (2, 1):
            for side in (0, 1):
                y_copy(block, side, 0, distance).start()

    def y_relay(block):
        for side in (block, 1 - block):
            y_copy(block, side, 2, 2).wait_recv()
            for distance in range(REACH[block][side], 2, -1):
                y_copy(block, side, 2, distance).start()

    def y_rest(block):
        for distance in (1, 3, 4):
            for side in (0, 1):
                if distance <= REACH[block][side]:
                    y_copy(block, side, distance, distance).wait_recv()

    states[y, xh, z] = e_ref[upper, z, quarter]
    for q in range(4):
        weights[z, xh, q] = w_ref[q * 64 : q * 64 + 64, pl.ds(pl.multiple_of(xh * 512, 512), 512)]
    acc[...] = jnp.zeros_like(acc)

    column = lax.broadcasted_iota(jnp.int32, (1, 1024), 1)
    lane = lax.rem(column, 128)
    by_owner = (
        (lane // 64) * 512
        + (lax.rem(lane, 64) // 16) * 128
        + (lax.rem(lane, 16) // 8) * 64
        + (column // 128) * 8
        + lax.rem(lane, 8)
    )
    by_head = (
        (lax.rem(lane, 64) // 8) * 128
        + (lax.rem(lane, 8) // 4) * 64
        + lax.rem(lane, 4) * 16
        + (lane // 64) * 8
        + column // 128
    )

    def build(i, carry):
        row = lax.broadcasted_iota(jnp.int32, (64, 1024), 0) + i * 64
        here = pl.ds(pl.multiple_of(i * 64, 64), 64)
        perm[here, :] = jnp.where(row == by_owner, 1.0, 0.0).astype(BF16)
        final[here, :] = jnp.where(row == by_head, 1.0, 0.0).astype(BF16)
        return carry

    lax.fori_loop(0, 16, build, 0)

    def multiply(block, distances):
        side = xh if block == 0 else other
        total = acc[...]
        for d in distances:
            i = turn(z, d)
            total = total + jnp.dot(
                states[:, side, i].reshape(128, 256), weights[i, side].reshape(256, 512),
                preferred_element_type=F32,
            )
        acc[...] = total

    def chip_take(phase, hops):
        for hop in hops:
            for short in (0, 1):
                for sub in (0, 1):
                    if hop < 4 or not short:
                        k = w_index(phase, hop, short, sub)
                        half = c if short else 1 - c
                        slot = weights.at[turn(z, way * hop), xh if phase == 0 else other, half * 2 + sub]
                        remote(slot, slot, chip_send.at[k], chip_recv.at[k], twin).wait_recv()

    w_take(0, 1, 0)
    w_take(0, 1, 1)
    take_states()
    e_far.start()
    y_own(0)
    w_take(0, 2, 0)
    w_take(0, 2, 1)
    far_own(0)
    far_own(1)
    w_take(0, 3, 0)
    twin_own()
    w_take(0, 3, 1)
    y_relay(0)
    w_take(0, 4, 0)
    e_far_in.wait_recv()
    y_own(1)
    w_take(1, 1, 0)
    w_take(1, 1, 1)
    w_take(1, 2, 0)
    w_take(1, 2, 1)
    w_take(1, 3, 0)
    y_relay(1)
    w_take(1, 3, 1)
    chip_take(0, (1, 2, 3, 4))
    y_rest(0)
    multiply(0, range(8))
    w_take(1, 4, 0)
    y_rest(1)
    chip_take(1, (1, 2))
    multiply(1, (0, 1, 2, 6, 7))
    len_load.wait()
    chip_take(1, (3, 4))
    multiply(1, (3, 4, 5))

    row = lax.broadcasted_iota(jnp.int32, (128, 512), 0)
    place = (row // 64) * 512 + z * 64 + lax.rem(row, 64)
    total = acc[...]
    kept = jnp.where(place < len_ref[0], total, jnp.zeros_like(total)).astype(BF16).reshape(2, 2, 32, 512)
    sorted_parts = jnp.dot(
        kept[:, 0].reshape(64, 512), perm[pl.ds(0, 512), :], preferred_element_type=F32
    ) + jnp.dot(kept[:, 1].reshape(64, 512), perm[pl.ds(512, 512), :], preferred_element_type=F32)
    sorted_parts = sorted_parts.astype(BF16)
    for b in (0, 1):
        for j in range(RING):
            parts[b * RING + j] = sorted_parts[b * 32 : b * 32 + 32, j * 128 : j * 128 + 128]

    e_far.wait_send()
    for sub in (0, 1):
        w_far[sub].wait_send()

    def sent(to, carry):
        @pl.when(to != z)
        def _():
            slot = states.at[y, xh, z]
            remote(slot, slot, e_send.at[to], e_recv.at[to], {"z": z}).wait_send()

        return carry

    lax.fori_loop(0, RING, sent, 0)
    for phase in (0, 1):
        for k in range(phase * 14, phase * 14 + 14):
            slot = weights.at[z, xh, 0]
            remote(slot, slot, z_send.at[k], z_recv.at[k], ahead).wait_send()
            remote(slot, slot, chip_send.at[k], chip_recv.at[k], twin).wait_send()
    for k in (28, 29):
        slot = weights.at[z, xh, 0]
        remote(slot, slot, chip_send.at[k], chip_recv.at[k], twin).wait_send()
    for block in (0, 1):
        for side in (0, 1):
            for distance in range(1, REACH[block][side] + 1):
                y_copy(block, side, 0, distance).wait_send()

    me = xh * RING + y

    for across in (1, 0):
        for dy in (4, 3, 5, 2, 6, 1, 7, 0):
            if across or dy:
                to_xh, to_y = (other if across else xh), turn(y, dy)
                remote(
                    parts.at[to_xh * RING + to_y], arrived.at[me], far_send.at[3], far_recv.at[3],
                    {"xh": to_xh, "y": to_y},
                ).start()
    arrived[me] = parts[me]
    most = arrived.at[pl.ds(0, 2 * RING - 1)]
    last = remote(most, most, far_send.at[3], far_recv.at[3], mate)
    last.wait_recv()
    rows = [
        jnp.concatenate(
            [arrived[s * RING + j][:, p * 64 : p * 64 + 64] for j in range(RING) for s in (0, 1)], axis=1
        )
        for p in (0, 1)
    ]
    out_ref[...] = jnp.dot(jnp.concatenate(rows, axis=0), final[...], preferred_element_type=F32).reshape(64, 8, 128).astype(BF16)
    last.wait_send()


def local(encoded, lengths, kv_weight):
    states = encoded.reshape(2, 8, 4, 16, 256)
    vmem = pl.BlockSpec(memory_space=pltpu.VMEM)
    hbm = pl.BlockSpec(memory_space=pltpu.HBM)
    keys_values = pl.pallas_call(
        project,
        out_shape=pltpu.VMEM((64, 8, 128), BF16),
        in_specs=[hbm, hbm, hbm],
        out_specs=vmem,
        scratch_shapes=[
            pltpu.SMEM((1,), jnp.int32),
            pltpu.VMEM((2, 8, 4, 16, 256), BF16),
            pltpu.VMEM((256, 8, 128), BF16),
            pltpu.VMEM((256, 1024), BF16),
            pltpu.VMEM((8, 2, 8, 16, 256), BF16),
            pltpu.VMEM((8, 2, 4, 64, 512), BF16),
            pltpu.VMEM((128, 512), F32),
            pltpu.VMEM((1024, 1024), BF16),
            pltpu.VMEM((1024, 1024), BF16),
            pltpu.VMEM((16, 32, 128), BF16),
            pltpu.VMEM((16, 32, 128), BF16),
            pltpu.SemaphoreType.DMA((6,)),
            pltpu.SemaphoreType.DMA((4,)),
            pltpu.SemaphoreType.DMA((4,)),
            pltpu.SemaphoreType.DMA((8,)),
            pltpu.SemaphoreType.DMA((8,)),
            pltpu.SemaphoreType.DMA((16,)),
            pltpu.SemaphoreType.DMA((16,)),
            pltpu.SemaphoreType.DMA((28,)),
            pltpu.SemaphoreType.DMA((28,)),
            pltpu.SemaphoreType.DMA((30,)),
            pltpu.SemaphoreType.DMA((30,)),
        ],
        compiler_params=pltpu.CompilerParams(collective_id=0, has_side_effects=True),
        name="project",
    )(states, lengths, kv_weight)
    return keys_values.reshape(1, 64, 8, 128)


def solution(mesh):
    torus = Mesh(mesh.devices.reshape(4, 2, 2, 8, 8), ("xl", "c", "xh", "z", "y"))
    placed = (P(("xl", "c"), None, ("xh", "z")), P(("xl", "c")), P(("xh", "z"), "y", None))
    return jax.shard_map(
        local, mesh=torus, in_specs=placed, out_specs=P(("xl", "c"), ("xh", "z"), "y", None), check_vma=False
    )
```

```python
import jax
import jax.numpy as jnp
from jax import lax
from jax.experimental import pallas as pl
from jax.experimental.pallas import tpu as pltpu
from jax.sharding import Mesh
from jax.sharding import PartitionSpec as P

MESH = pl.DeviceIdType.MESH
RING = 8
BF16 = jnp.bfloat16
F32 = jnp.float32


def project(
    e_in, len_in, w_in, out_ref,
    len_ref, e_ref, w_raw, w_ref, states, weights, acc, perm, final, parts, arrived,
    load, far_send, far_recv, e_send, e_recv, y_send, y_recv, z_send, z_recv, chip_send, chip_recv,
):
    xh, z, y, c = (lax.axis_index(a) for a in ("xh", "z", "y", "c"))
    other = 1 - xh
    mate = {"xh": other}
    twin = {"c": 1 - c}
    upper, quarter = y // 4, lax.rem(y, 4)

    def turn(base, by):
        return lax.rem(base + by + 2 * RING, RING)

    def remote(src, dst, send, recv, to):
        return pltpu.make_async_remote_copy(
            src_ref=src, dst_ref=dst, send_sem=send, recv_sem=recv, device_id=to, device_id_type=MESH
        )

    def signal(sem, to):
        pl.semaphore_signal(sem, inc=1, device_id=to, device_id_type=MESH)

    def rows_of(q):
        half = c if q < 2 else 1 - c
        return pl.ds(pl.multiple_of(half * 128 + (q % 2) * 64, 64), 64)

    w_load = [pltpu.make_async_copy(w_in.at[rows_of(q)], w_raw.at[rows_of(q)], load.at[q]) for q in range(4)]
    e_load = pltpu.make_async_copy(e_in, e_ref, load.at[4])
    len_load = pltpu.make_async_copy(len_in, len_ref, load.at[5])
    w_load[0].start()
    w_load[1].start()
    e_load.start()
    w_load[2].start()
    w_load[3].start()
    len_load.start()

    barrier = pltpu.get_barrier_semaphore()

    def greet(i, carry):
        signal(barrier, {"z": turn(z, i)})
        return carry

    lax.fori_loop(1, RING, greet, 0)
    for dy in (1, -1, 2, -2):
        signal(barrier, {"y": turn(y, dy)})
    signal(barrier, mate)
    signal(barrier, twin)

    def lay_out(q):
        w_load[q].wait()
        for e in range(8):
            w_ref[rows_of(q), e * 128 : e * 128 + 128] = w_raw[rows_of(q), e, :]

    lay_out(0)
    lay_out(1)
    pl.semaphore_wait(barrier, RING - 1 + 6)

    def far_weights(sub):
        return remote(
            w_ref.at[pl.ds(c * 128 + sub * 64, 64), pl.ds(pl.multiple_of(other * 512, 512), 512)],
            weights.at[z, xh, c * 2 + sub], far_send.at[1 + sub], far_recv.at[1 + sub], mate,
        )

    w_far = [far_weights(sub) for sub in (0, 1)]
    e_far = remote(states.at[y, xh], states.at[y, xh], far_send.at[0], far_recv.at[0], mate)
    e_far_in = remote(states.at[y, other], states.at[y, other], far_send.at[0], far_recv.at[0], mate)
    w_far[0].start()
    w_far[1].start()

    way = 1 - 2 * c
    next_z = turn(z, way)
    ahead = {"z": next_z}

    def w_slot(phase, hop, short, sub):
        source = turn(z, -way * hop)
        half = 1 - c if short else c
        return weights.at[source, xh if phase == 0 else other, half * 2 + sub]

    def w_index(phase, hop, short, sub):
        return phase * 14 + (hop - 1) * 4 + short * 2 + sub

    def w_send(phase, hop, short, sub, src):
        k = w_index(phase, hop + 1, short, sub)
        remote(src, w_slot(phase, hop, short, sub), z_send.at[k], z_recv.at[k], ahead).start()

    def w_take(phase, hop, short):
        for sub in (0, 1):
            k = w_index(phase, hop, short, sub)
            slot = w_slot(phase, hop, short, sub)
            remote(slot, slot, z_send.at[k], z_recv.at[k], ahead).wait_recv()
            if hop < 3 or (hop == 3 and not short):
                w_send(phase, hop, short, sub, slot)
            remote(slot, slot, chip_send.at[k], chip_recv.at[k], twin).start()

    def own_weight(short):
        half = 1 - c if short else c
        for sub in (0, 1):
            w_send(
                0, 0, short, sub,
                w_ref.at[pl.ds(half * 128 + sub * 64, 64), pl.ds(pl.multiple_of(xh * 512, 512), 512)],
            )

    def far_own(sub):
        slot = weights.at[z, other, c * 2 + sub]
        remote(slot, slot, far_send.at[1 + sub], far_recv.at[1 + sub], mate).wait_recv()
        w_send(1, 0, 0, sub, slot)
        remote(slot, slot, chip_send.at[28 + sub], chip_recv.at[28 + sub], twin).start()

    def twin_own():
        for sub in (0, 1):
            slot = weights.at[z, other, (1 - c) * 2 + sub]
            remote(slot, slot, chip_send.at[28 + sub], chip_recv.at[28 + sub], twin).wait_recv()
            w_send(1, 0, 1, sub, slot)

    e_load.wait()

    def spread(to, carry):
        @pl.when(to != z)
        def _():
            remote(
                e_ref.at[upper, to, quarter], states.at[y, xh, z], e_send.at[to], e_recv.at[z], {"z": to}
            ).start()

        return carry

    def take_states():
        def one(source, carry):
            @pl.when(source != z)
            def _():
                slot = states.at[y, xh, source]
                remote(slot, slot, e_send.at[source], e_recv.at[source], {"z": z}).wait_recv()

            return carry

        lax.fori_loop(0, RING, one, 0)

    lax.fori_loop(0, RING, spread, 0)
    own_weight(0)
    lay_out(2)
    lay_out(3)
    own_weight(1)

    REACH = ((4, 3), (3, 4))

    def y_index(block, side, distance):
        return (block * 2 + side) * 4 + distance - 1

    def y_copy(block, side, origin, distance):
        sign = 1 if side == 0 else -1
        slot = states.at[turn(y, -sign * origin), xh if block == 0 else other]
        k = y_index(block, side, distance)
        return remote(slot, slot, y_send.at[k], y_recv.at[k], {"y": turn(y, sign * (distance - origin))})

    def y_own(block):
        for distance in (2, 1):
            for side in (0, 1):
                y_copy(block, side, 0, distance).start()

    def y_relay(block):
        for side in (block, 1 - block):
            y_copy(block, side, 2, 2).wait_recv()
            for distance in range(REACH[block][side], 2, -1):
                y_copy(block, side, 2, distance).start()

    def y_rest(block):
        for distance in (1, 3, 4):
            for side in (0, 1):
                if distance <= REACH[block][side]:
                    y_copy(block, side, distance, distance).wait_recv()

    states[y, xh, z] = e_ref[upper, z, quarter]
    for q in range(4):
        weights[z, xh, q] = w_ref[q * 64 : q * 64 + 64, pl.ds(pl.multiple_of(xh * 512, 512), 512)]
    acc[...] = jnp.zeros_like(acc)

    column = lax.broadcasted_iota(jnp.int32, (1, 1024), 1)
    lane = lax.rem(column, 128)
    by_owner = (
        (lane // 64) * 512
        + (lax.rem(lane, 64) // 16) * 128
        + (lax.rem(lane, 16) // 8) * 64
        + (column // 128) * 8
        + lax.rem(lane, 8)
    )
    by_head = (
        (lax.rem(lane, 64) // 8) * 128
        + (lax.rem(lane, 8) // 4) * 64
        + lax.rem(lane, 4) * 16
        + (lane // 64) * 8
        + column // 128
    )

    def build(i, carry):
        row = lax.broadcasted_iota(jnp.int32, (64, 1024), 0) + i * 64
        here = pl.ds(pl.multiple_of(i * 64, 64), 64)
        perm[here, :] = jnp.where(row == by_owner, 1.0, 0.0).astype(BF16)
        final[here, :] = jnp.where(row == by_head, 1.0, 0.0).astype(BF16)
        return carry

    lax.fori_loop(0, 16, build, 0)

    def multiply(block, distances):
        side = xh if block == 0 else other
        total = acc[...]
        for d in distances:
            i = turn(z, d)
            total = total + jnp.dot(
                states[:, side, i].reshape(128, 256), weights[i, side].reshape(256, 512),
                preferred_element_type=F32,
            )
        acc[...] = total

    def chip_take(phase, hops):
        for hop in hops:
            for short in (0, 1):
                for sub in (0, 1):
                    if hop < 4 or not short:
                        k = w_index(phase, hop, short, sub)
                        half = c if short else 1 - c
                        slot = weights.at[turn(z, way * hop), xh if phase == 0 else other, half * 2 + sub]
                        remote(slot, slot, chip_send.at[k], chip_recv.at[k], twin).wait_recv()

    w_take(0, 1, 0)
    w_take(0, 1, 1)
    take_states()
    e_far.start()
    y_own(0)
    w_take(0, 2, 0)
    w_take(0, 2, 1)
    far_own(0)
    far_own(1)
    w_take(0, 3, 0)
    twin_own()
    y_relay(0)
    w_take(1, 1, 0)
    e_far_in.wait_recv()
    y_own(1)
    w_take(1, 1, 1)
    w_take(1, 2, 0)
    w_take(1, 2, 1)
    w_take(1, 3, 0)
    y_relay(1)
    w_take(0, 3, 1)
    w_take(0, 4, 0)
    w_take(1, 3, 1)
    chip_take(0, (1, 2, 3, 4))
    y_rest(0)
    multiply(0, range(8))
    w_take(1, 4, 0)
    y_rest(1)
    chip_take(1, (1, 2))
    multiply(1, (0, 1, 2, 6, 7))
    len_load.wait()
    chip_take(1, (3, 4))
    multiply(1, (3, 4, 5))

    row = lax.broadcasted_iota(jnp.int32, (128, 512), 0)
    place = (row // 64) * 512 + z * 64 + lax.rem(row, 64)
    total = acc[...]
    kept = jnp.where(place < len_ref[0], total, jnp.zeros_like(total)).astype(BF16).reshape(2, 2, 32, 512)
    sorted_parts = jnp.dot(
        kept[:, 0].reshape(64, 512), perm[pl.ds(0, 512), :], preferred_element_type=F32
    ) + jnp.dot(kept[:, 1].reshape(64, 512), perm[pl.ds(512, 512), :], preferred_element_type=F32)
    sorted_parts = sorted_parts.astype(BF16)
    for b in (0, 1):
        for j in range(RING):
            parts[b * RING + j] = sorted_parts[b * 32 : b * 32 + 32, j * 128 : j * 128 + 128]

    e_far.wait_send()
    for sub in (0, 1):
        w_far[sub].wait_send()

    def sent(to, carry):
        @pl.when(to != z)
        def _():
            slot = states.at[y, xh, z]
            remote(slot, slot, e_send.at[to], e_recv.at[to], {"z": z}).wait_send()

        return carry

    lax.fori_loop(0, RING, sent, 0)
    for block in (0, 1):
        for side in (0, 1):
            for distance in range(1, REACH[block][side] + 1):
                y_copy(block, side, 0, distance).wait_send()

    me = xh * RING + y

    for across in (1, 0):
        for dy in (4, 3, 5, 2, 6, 1, 7, 0):
            if across or dy:
                to_xh, to_y = (other if across else xh), turn(y, dy)
                remote(
                    parts.at[to_xh * RING + to_y], arrived.at[me], far_send.at[3], far_recv.at[3],
                    {"xh": to_xh, "y": to_y},
                ).start()
    arrived[me] = parts[me]
    for phase in (0, 1):
        for k in range(phase * 14, phase * 14 + 14):
            slot = weights.at[z, xh, 0]
            remote(slot, slot, z_send.at[k], z_recv.at[k], ahead).wait_send()
            remote(slot, slot, chip_send.at[k], chip_recv.at[k], twin).wait_send()
    for k in (28, 29):
        slot = weights.at[z, xh, 0]
        remote(slot, slot, chip_send.at[k], chip_recv.at[k], twin).wait_send()
    most = arrived.at[pl.ds(0, 2 * RING - 1)]
    last = remote(most, most, far_send.at[3], far_recv.at[3], mate)
    last.wait_recv()
    rows = [
        jnp.concatenate(
            [arrived[s * RING + j][:, p * 64 : p * 64 + 64] for j in range(RING) for s in (0, 1)], axis=1
        )
        for p in (0, 1)
    ]
    out_ref[...] = jnp.dot(jnp.concatenate(rows, axis=0), final[...], preferred_element_type=F32).reshape(64, 8, 128).astype(BF16)
    last.wait_send()


def local(encoded, lengths, kv_weight):
    states = encoded.reshape(2, 8, 4, 16, 256)
    vmem = pl.BlockSpec(memory_space=pltpu.VMEM)
    hbm = pl.BlockSpec(memory_space=pltpu.HBM)
    keys_values = pl.pallas_call(
        project,
        out_shape=pltpu.VMEM((64, 8, 128), BF16),
        in_specs=[hbm, hbm, hbm],
        out_specs=vmem,
        scratch_shapes=[
            pltpu.SMEM((1,), jnp.int32),
            pltpu.VMEM((2, 8, 4, 16, 256), BF16),
            pltpu.VMEM((256, 8, 128), BF16),
            pltpu.VMEM((256, 1024), BF16),
            pltpu.VMEM((8, 2, 8, 16, 256), BF16),
            pltpu.VMEM((8, 2, 4, 64, 512), BF16),
            pltpu.VMEM((128, 512), F32),
            pltpu.VMEM((1024, 1024), BF16),
            pltpu.VMEM((1024, 1024), BF16),
            pltpu.VMEM((16, 32, 128), BF16),
            pltpu.VMEM((16, 32, 128), BF16),
            pltpu.SemaphoreType.DMA((6,)),
            pltpu.SemaphoreType.DMA((4,)),
            pltpu.SemaphoreType.DMA((4,)),
            pltpu.SemaphoreType.DMA((8,)),
            pltpu.SemaphoreType.DMA((8,)),
            pltpu.SemaphoreType.DMA((16,)),
            pltpu.SemaphoreType.DMA((16,)),
            pltpu.SemaphoreType.DMA((28,)),
            pltpu.SemaphoreType.DMA((28,)),
            pltpu.SemaphoreType.DMA((30,)),
            pltpu.SemaphoreType.DMA((30,)),
        ],
        compiler_params=pltpu.CompilerParams(collective_id=0, has_side_effects=True),
        name="project",
    )(states, lengths, kv_weight)
    return keys_values.reshape(1, 64, 8, 128)


def solution(mesh):
    torus = Mesh(mesh.devices.reshape(4, 2, 2, 8, 8), ("xl", "c", "xh", "z", "y"))
    placed = (P(("xl", "c"), None, ("xh", "z")), P(("xl", "c")), P(("xh", "z"), "y", None))
    return jax.shard_map(
        local, mesh=torus, in_specs=placed, out_specs=P(("xl", "c"), ("xh", "z"), "y", None), check_vma=False
    )
```

```python
import jax
import jax.numpy as jnp
from jax import lax
from jax.experimental import pallas as pl
from jax.experimental.pallas import tpu as pltpu
from jax.sharding import Mesh
from jax.sharding import PartitionSpec as P

MESH = pl.DeviceIdType.MESH
RING = 8
BF16 = jnp.bfloat16
F32 = jnp.float32


def project(
    e_in, len_in, w_in, out_ref,
    len_ref, e_ref, w_raw, w_ref, states, weights, acc, perm, final, parts, arrived,
    load, far_send, far_recv, e_send, e_recv, y_send, y_recv, z_send, z_recv, chip_send, chip_recv,
):
    xh, z, y, c = (lax.axis_index(a) for a in ("xh", "z", "y", "c"))
    other = 1 - xh
    mate = {"xh": other}
    twin = {"c": 1 - c}
    upper, quarter = y // 4, lax.rem(y, 4)

    def turn(base, by):
        return lax.rem(base + by + 2 * RING, RING)

    def remote(src, dst, send, recv, to):
        return pltpu.make_async_remote_copy(
            src_ref=src, dst_ref=dst, send_sem=send, recv_sem=recv, device_id=to, device_id_type=MESH
        )

    def signal(sem, to):
        pl.semaphore_signal(sem, inc=1, device_id=to, device_id_type=MESH)

    def rows_of(q):
        half = c if q < 2 else 1 - c
        return pl.ds(pl.multiple_of(half * 128 + (q % 2) * 64, 64), 64)

    w_load = [pltpu.make_async_copy(w_in.at[rows_of(q)], w_raw.at[rows_of(q)], load.at[q]) for q in range(4)]
    e_load = pltpu.make_async_copy(e_in, e_ref, load.at[4])
    len_load = pltpu.make_async_copy(len_in, len_ref, load.at[5])
    w_load[0].start()
    w_load[1].start()
    e_load.start()
    w_load[2].start()
    w_load[3].start()
    len_load.start()

    barrier = pltpu.get_barrier_semaphore()

    def greet(i, carry):
        signal(barrier, {"z": turn(z, i)})
        return carry

    lax.fori_loop(1, RING, greet, 0)
    for dy in (1, -1, 2, -2):
        signal(barrier, {"y": turn(y, dy)})
    signal(barrier, mate)
    signal(barrier, twin)

    def lay_out(q):
        w_load[q].wait()
        for e in range(8):
            w_ref[rows_of(q), e * 128 : e * 128 + 128] = w_raw[rows_of(q), e, :]

    lay_out(0)
    lay_out(1)
    pl.semaphore_wait(barrier, RING - 1 + 6)

    def far_weights(sub):
        return remote(
            w_ref.at[pl.ds(c * 128 + sub * 64, 64), pl.ds(pl.multiple_of(other * 512, 512), 512)],
            weights.at[z, xh, c * 2 + sub], far_send.at[1 + sub], far_recv.at[1 + sub], mate,
        )

    w_far = [far_weights(sub) for sub in (0, 1)]
    e_far = remote(states.at[y, xh], states.at[y, xh], far_send.at[0], far_recv.at[0], mate)
    e_far_in = remote(states.at[y, other], states.at[y, other], far_send.at[0], far_recv.at[0], mate)
    w_far[0].start()
    w_far[1].start()

    way = 1 - 2 * c
    next_z = turn(z, way)
    ahead = {"z": next_z}

    def w_slot(phase, hop, short, sub):
        source = turn(z, -way * hop)
        half = 1 - c if short else c
        return weights.at[source, xh if phase == 0 else other, half * 2 + sub]

    def w_index(phase, hop, short, sub):
        return phase * 14 + (hop - 1) * 4 + short * 2 + sub

    def w_send(phase, hop, short, sub, src):
        k = w_index(phase, hop + 1, short, sub)
        remote(src, w_slot(phase, hop, short, sub), z_send.at[k], z_recv.at[k], ahead).start()

    def w_take(phase, hop, short):
        for sub in (0, 1):
            k = w_index(phase, hop, short, sub)
            slot = w_slot(phase, hop, short, sub)
            remote(slot, slot, z_send.at[k], z_recv.at[k], ahead).wait_recv()
            if hop < 3 or (hop == 3 and not short):
                w_send(phase, hop, short, sub, slot)
            remote(slot, slot, chip_send.at[k], chip_recv.at[k], twin).start()

    def own_weight(short):
        half = 1 - c if short else c
        for sub in (0, 1):
            w_send(
                0, 0, short, sub,
                w_ref.at[pl.ds(half * 128 + sub * 64, 64), pl.ds(pl.multiple_of(xh * 512, 512), 512)],
            )

    def far_own(sub):
        slot = weights.at[z, other, c * 2 + sub]
        remote(slot, slot, far_send.at[1 + sub], far_recv.at[1 + sub], mate).wait_recv()
        w_send(1, 0, 0, sub, slot)
        remote(slot, slot, chip_send.at[28 + sub], chip_recv.at[28 + sub], twin).start()

    def twin_own():
        for sub in (0, 1):
            slot = weights.at[z, other, (1 - c) * 2 + sub]
            remote(slot, slot, chip_send.at[28 + sub], chip_recv.at[28 + sub], twin).wait_recv()
            w_send(1, 0, 1, sub, slot)

    e_load.wait()

    def spread(to, carry):
        @pl.when(to != z)
        def _():
            remote(
                e_ref.at[upper, to, quarter], states.at[y, xh, z], e_send.at[to], e_recv.at[z], {"z": to}
            ).start()

        return carry

    def take_states():
        def one(source, carry):
            @pl.when(source != z)
            def _():
                slot = states.at[y, xh, source]
                remote(slot, slot, e_send.at[source], e_recv.at[source], {"z": z}).wait_recv()

            return carry

        lax.fori_loop(0, RING, one, 0)

    lax.fori_loop(0, RING, spread, 0)
    own_weight(0)
    lay_out(2)
    lay_out(3)
    own_weight(1)

    REACH = ((4, 3), (3, 4))

    def y_index(block, side, distance):
        return (block * 2 + side) * 4 + distance - 1

    def y_copy(block, side, origin, distance):
        sign = 1 if side == 0 else -1
        slot = states.at[turn(y, -sign * origin), xh if block == 0 else other]
        k = y_index(block, side, distance)
        return remote(slot, slot, y_send.at[k], y_recv.at[k], {"y": turn(y, sign * (distance - origin))})

    def y_own(block):
        for distance in (2, 1):
            for side in (0, 1):
                y_copy(block, side, 0, distance).start()

    def y_relay(block):
        for side in (block, 1 - block):
            y_copy(block, side, 2, 2).wait_recv()
            for distance in range(REACH[block][side], 2, -1):
                y_copy(block, side, 2, distance).start()

    def y_rest(block):
        for distance in (1, 3, 4):
            for side in (0, 1):
                if distance <= REACH[block][side]:
                    y_copy(block, side, distance, distance).wait_recv()

    states[y, xh, z] = e_ref[upper, z, quarter]
    for q in range(4):
        weights[z, xh, q] = w_ref[q * 64 : q * 64 + 64, pl.ds(pl.multiple_of(xh * 512, 512), 512)]
    acc[...] = jnp.zeros_like(acc)

    column = lax.broadcasted_iota(jnp.int32, (1, 1024), 1)
    lane = lax.rem(column, 128)
    by_owner = (
        (lane // 64) * 512
        + (lax.rem(lane, 64) // 16) * 128
        + (lax.rem(lane, 16) // 8) * 64
        + (column // 128) * 8
        + lax.rem(lane, 8)
    )
    by_head = (
        (lax.rem(lane, 64) // 8) * 128
        + (lax.rem(lane, 8) // 4) * 64
        + lax.rem(lane, 4) * 16
        + (lane // 64) * 8
        + column // 128
    )

    def build(i, carry):
        row = lax.broadcasted_iota(jnp.int32, (64, 1024), 0) + i * 64
        here = pl.ds(pl.multiple_of(i * 64, 64), 64)
        perm[here, :] = jnp.where(row == by_owner, 1.0, 0.0).astype(BF16)
        final[here, :] = jnp.where(row == by_head, 1.0, 0.0).astype(BF16)
        return carry

    lax.fori_loop(0, 16, build, 0)

    def multiply(block, distances):
        side = xh if block == 0 else other
        total = acc[...]
        for d in distances:
            i = turn(z, d)
            total = total + jnp.dot(
                states[:, side, i].reshape(128, 256), weights[i, side].reshape(256, 512),
                preferred_element_type=F32,
            )
        acc[...] = total

    def chip_take(phase, hops):
        for hop in hops:
            for short in (0, 1):
                for sub in (0, 1):
                    if hop < 4 or not short:
                        k = w_index(phase, hop, short, sub)
                        half = c if short else 1 - c
                        slot = weights.at[turn(z, way * hop), xh if phase == 0 else other, half * 2 + sub]
                        remote(slot, slot, chip_send.at[k], chip_recv.at[k], twin).wait_recv()

    w_take(0, 1, 0)
    w_take(0, 1, 1)
    take_states()
    e_far.start()
    y_own(0)
    w_take(0, 2, 0)
    w_take(0, 2, 1)
    far_own(0)
    far_own(1)
    w_take(0, 3, 0)
    twin_own()
    y_relay(0)
    e_far_in.wait_recv()
    y_own(1)
    w_take(1, 1, 0)
    w_take(1, 1, 1)
    w_take(1, 2, 0)
    w_take(1, 2, 1)
    w_take(1, 3, 0)
    y_relay(1)
    w_take(0, 3, 1)
    w_take(0, 4, 0)
    w_take(1, 3, 1)
    w_take(1, 4, 0)
    chip_take(0, (1, 2, 3, 4))
    y_rest(0)
    multiply(0, range(8))
    y_rest(1)
    chip_take(1, (1, 2))
    multiply(1, (0, 1, 2, 6, 7))
    len_load.wait()
    chip_take(1, (3, 4))
    multiply(1, (3, 4, 5))

    row = lax.broadcasted_iota(jnp.int32, (128, 512), 0)
    place = (row // 64) * 512 + z * 64 + lax.rem(row, 64)
    total = acc[...]
    kept = jnp.where(place < len_ref[0], total, jnp.zeros_like(total)).astype(BF16).reshape(2, 2, 32, 512)
    sorted_parts = jnp.dot(
        kept[:, 0].reshape(64, 512), perm[pl.ds(0, 512), :], preferred_element_type=F32
    ) + jnp.dot(kept[:, 1].reshape(64, 512), perm[pl.ds(512, 512), :], preferred_element_type=F32)
    sorted_parts = sorted_parts.astype(BF16)
    for b in (0, 1):
        for j in range(RING):
            parts[b * RING + j] = sorted_parts[b * 32 : b * 32 + 32, j * 128 : j * 128 + 128]

    e_far.wait_send()
    for sub in (0, 1):
        w_far[sub].wait_send()

    def sent(to, carry):
        @pl.when(to != z)
        def _():
            slot = states.at[y, xh, z]
            remote(slot, slot, e_send.at[to], e_recv.at[to], {"z": z}).wait_send()

        return carry

    lax.fori_loop(0, RING, sent, 0)
    for block in (0, 1):
        for side in (0, 1):
            for distance in range(1, REACH[block][side] + 1):
                y_copy(block, side, 0, distance).wait_send()

    me = xh * RING + y

    for across in (1, 0):
        for dy in (4, 3, 5, 2, 6, 1, 7, 0):
            if across or dy:
                to_xh, to_y = (other if across else xh), turn(y, dy)
                remote(
                    parts.at[to_xh * RING + to_y], arrived.at[me], far_send.at[3], far_recv.at[3],
                    {"xh": to_xh, "y": to_y},
                ).start()
    arrived[me] = parts[me]
    for phase in (0, 1):
        for k in range(phase * 14, phase * 14 + 14):
            slot = weights.at[z, xh, 0]
            remote(slot, slot, z_send.at[k], z_recv.at[k], ahead).wait_send()
            remote(slot, slot, chip_send.at[k], chip_recv.at[k], twin).wait_send()
    for k in (28, 29):
        slot = weights.at[z, xh, 0]
        remote(slot, slot, chip_send.at[k], chip_recv.at[k], twin).wait_send()
    most = arrived.at[pl.ds(0, 2 * RING - 1)]
    last = remote(most, most, far_send.at[3], far_recv.at[3], mate)
    last.wait_recv()
    rows = [
        jnp.concatenate(
            [arrived[s * RING + j][:, p * 64 : p * 64 + 64] for j in range(RING) for s in (0, 1)], axis=1
        )
        for p in (0, 1)
    ]
    out_ref[...] = jnp.dot(jnp.concatenate(rows, axis=0), final[...], preferred_element_type=F32).reshape(64, 8, 128).astype(BF16)
    last.wait_send()


def local(encoded, lengths, kv_weight):
    states = encoded.reshape(2, 8, 4, 16, 256)
    vmem = pl.BlockSpec(memory_space=pltpu.VMEM)
    hbm = pl.BlockSpec(memory_space=pltpu.HBM)
    keys_values = pl.pallas_call(
        project,
        out_shape=pltpu.VMEM((64, 8, 128), BF16),
        in_specs=[hbm, hbm, hbm],
        out_specs=vmem,
        scratch_shapes=[
            pltpu.SMEM((1,), jnp.int32),
            pltpu.VMEM((2, 8, 4, 16, 256), BF16),
            pltpu.VMEM((256, 8, 128), BF16),
            pltpu.VMEM((256, 1024), BF16),
            pltpu.VMEM((8, 2, 8, 16, 256), BF16),
            pltpu.VMEM((8, 2, 4, 64, 512), BF16),
            pltpu.VMEM((128, 512), F32),
            pltpu.VMEM((1024, 1024), BF16),
            pltpu.VMEM((1024, 1024), BF16),
            pltpu.VMEM((16, 32, 128), BF16),
            pltpu.VMEM((16, 32, 128), BF16),
            pltpu.SemaphoreType.DMA((6,)),
            pltpu.SemaphoreType.DMA((4,)),
            pltpu.SemaphoreType.DMA((4,)),
            pltpu.SemaphoreType.DMA((8,)),
            pltpu.SemaphoreType.DMA((8,)),
            pltpu.SemaphoreType.DMA((16,)),
            pltpu.SemaphoreType.DMA((16,)),
            pltpu.SemaphoreType.DMA((28,)),
            pltpu.SemaphoreType.DMA((28,)),
            pltpu.SemaphoreType.DMA((30,)),
            pltpu.SemaphoreType.DMA((30,)),
        ],
        compiler_params=pltpu.CompilerParams(collective_id=0, has_side_effects=True),
        name="project",
    )(states, lengths, kv_weight)
    return keys_values.reshape(1, 64, 8, 128)


def solution(mesh):
    torus = Mesh(mesh.devices.reshape(4, 2, 2, 8, 8), ("xl", "c", "xh", "z", "y"))
    placed = (P(("xl", "c"), None, ("xh", "z")), P(("xl", "c")), P(("xh", "z"), "y", None))
    return jax.shard_map(
        local, mesh=torus, in_specs=placed, out_specs=P(("xl", "c"), ("xh", "z"), "y", None), check_vma=False
    )
```

```python
import jax
import jax.numpy as jnp
from jax import lax
from jax.experimental import pallas as pl
from jax.experimental.pallas import tpu as pltpu
from jax.sharding import Mesh
from jax.sharding import PartitionSpec as P

MESH = pl.DeviceIdType.MESH
RING = 8
BF16 = jnp.bfloat16
F32 = jnp.float32


def project(
    e_in, len_in, w_in, out_ref,
    len_ref, e_ref, w_raw, w_ref, states, weights, acc, perm, final, parts, arrived,
    load, far_send, far_recv, e_send, e_recv, y_send, y_recv, z_send, z_recv, chip_send, chip_recv,
):
    xh, z, y, c = (lax.axis_index(a) for a in ("xh", "z", "y", "c"))
    other = 1 - xh
    mate = {"xh": other}
    twin = {"c": 1 - c}
    upper, quarter = y // 4, lax.rem(y, 4)

    def turn(base, by):
        return lax.rem(base + by + 2 * RING, RING)

    def remote(src, dst, send, recv, to):
        return pltpu.make_async_remote_copy(
            src_ref=src, dst_ref=dst, send_sem=send, recv_sem=recv, device_id=to, device_id_type=MESH
        )

    def signal(sem, to):
        pl.semaphore_signal(sem, inc=1, device_id=to, device_id_type=MESH)

    def rows_of(q):
        half = c if q < 2 else 1 - c
        return pl.ds(pl.multiple_of(half * 128 + (q % 2) * 64, 64), 64)

    w_load = [pltpu.make_async_copy(w_in.at[rows_of(q)], w_raw.at[rows_of(q)], load.at[q]) for q in range(4)]
    e_load = pltpu.make_async_copy(e_in, e_ref, load.at[4])
    len_load = pltpu.make_async_copy(len_in, len_ref, load.at[5])
    w_load[0].start()
    w_load[1].start()
    e_load.start()
    w_load[2].start()
    w_load[3].start()
    len_load.start()

    barrier = pltpu.get_barrier_semaphore()

    def greet(i, carry):
        signal(barrier, {"z": turn(z, i)})
        return carry

    lax.fori_loop(1, RING, greet, 0)
    for dy in (1, -1, 2, -2):
        signal(barrier, {"y": turn(y, dy)})
    signal(barrier, mate)
    signal(barrier, twin)

    def lay_out(q):
        w_load[q].wait()
        for e in range(8):
            w_ref[rows_of(q), e * 128 : e * 128 + 128] = w_raw[rows_of(q), e, :]

    lay_out(0)
    lay_out(1)
    pl.semaphore_wait(barrier, RING - 1 + 6)

    def far_weights(sub):
        return remote(
            w_ref.at[pl.ds(c * 128 + sub * 64, 64), pl.ds(pl.multiple_of(other * 512, 512), 512)],
            weights.at[z, xh, c * 2 + sub], far_send.at[1 + sub], far_recv.at[1 + sub], mate,
        )

    w_far = [far_weights(sub) for sub in (0, 1)]
    e_far = remote(states.at[y, xh], states.at[y, xh], far_send.at[0], far_recv.at[0], mate)
    e_far_in = remote(states.at[y, other], states.at[y, other], far_send.at[0], far_recv.at[0], mate)
    w_far[0].start()
    w_far[1].start()

    way = 1 - 2 * c
    next_z = turn(z, way)
    ahead = {"z": next_z}

    def w_slot(phase, hop, short, sub):
        source = turn(z, -way * hop)
        half = 1 - c if short else c
        return weights.at[source, xh if phase == 0 else other, half * 2 + sub]

    def w_index(phase, hop, short, sub):
        return phase * 14 + (hop - 1) * 4 + short * 2 + sub

    def w_send(phase, hop, short, sub, src):
        k = w_index(phase, hop + 1, short, sub)
        remote(src, w_slot(phase, hop, short, sub), z_send.at[k], z_recv.at[k], ahead).start()

    def w_take(phase, hop, short):
        for sub in (0, 1):
            k = w_index(phase, hop, short, sub)
            slot = w_slot(phase, hop, short, sub)
            remote(slot, slot, z_send.at[k], z_recv.at[k], ahead).wait_recv()
            if hop < 3 or (hop == 3 and not short):
                w_send(phase, hop, short, sub, slot)
            remote(slot, slot, chip_send.at[k], chip_recv.at[k], twin).start()

    def own_weight(short):
        half = 1 - c if short else c
        for sub in (0, 1):
            w_send(
                0, 0, short, sub,
                w_ref.at[pl.ds(half * 128 + sub * 64, 64), pl.ds(pl.multiple_of(xh * 512, 512), 512)],
            )

    def far_own(sub):
        slot = weights.at[z, other, c * 2 + sub]
        remote(slot, slot, far_send.at[1 + sub], far_recv.at[1 + sub], mate).wait_recv()
        w_send(1, 0, 0, sub, slot)
        remote(slot, slot, chip_send.at[28 + sub], chip_recv.at[28 + sub], twin).start()

    def twin_own():
        for sub in (0, 1):
            slot = weights.at[z, other, (1 - c) * 2 + sub]
            remote(slot, slot, chip_send.at[28 + sub], chip_recv.at[28 + sub], twin).wait_recv()
            w_send(1, 0, 1, sub, slot)

    e_load.wait()

    def spread(to, carry):
        @pl.when(to != z)
        def _():
            remote(
                e_ref.at[upper, to, quarter], states.at[y, xh, z], e_send.at[to], e_recv.at[z], {"z": to}
            ).start()

        return carry

    def take_states():
        def one(source, carry):
            @pl.when(source != z)
            def _():
                slot = states.at[y, xh, source]
                remote(slot, slot, e_send.at[source], e_recv.at[source], {"z": z}).wait_recv()

            return carry

        lax.fori_loop(0, RING, one, 0)

    lax.fori_loop(0, RING, spread, 0)
    own_weight(0)
    lay_out(2)
    lay_out(3)
    own_weight(1)

    REACH = ((4, 3), (3, 4))

    def y_index(block, side, distance):
        return (block * 2 + side) * 4 + distance - 1

    def y_copy(block, side, origin, distance):
        sign = 1 if side == 0 else -1
        slot = states.at[turn(y, -sign * origin), xh if block == 0 else other]
        k = y_index(block, side, distance)
        return remote(slot, slot, y_send.at[k], y_recv.at[k], {"y": turn(y, sign * (distance - origin))})

    def y_own(block):
        for distance in (2, 1):
            for side in (0, 1):
                y_copy(block, side, 0, distance).start()

    def y_relay(block):
        for side in (block, 1 - block):
            y_copy(block, side, 2, 2).wait_recv()
            for distance in range(REACH[block][side], 2, -1):
                y_copy(block, side, 2, distance).start()

    def y_rest(block):
        for distance in (1, 3, 4):
            for side in (0, 1):
                if distance <= REACH[block][side]:
                    y_copy(block, side, distance, distance).wait_recv()

    states[y, xh, z] = e_ref[upper, z, quarter]
    for q in range(4):
        weights[z, xh, q] = w_ref[q * 64 : q * 64 + 64, pl.ds(pl.multiple_of(xh * 512, 512), 512)]
    acc[...] = jnp.zeros_like(acc)

    column = lax.broadcasted_iota(jnp.int32, (1, 1024), 1)
    lane = lax.rem(column, 128)
    by_owner = (
        (lane // 64) * 512
        + (lax.rem(lane, 64) // 16) * 128
        + (lax.rem(lane, 16) // 8) * 64
        + (column // 128) * 8
        + lax.rem(lane, 8)
    )
    by_head = (
        (lax.rem(lane, 64) // 8) * 128
        + (lax.rem(lane, 8) // 4) * 64
        + lax.rem(lane, 4) * 16
        + (lane // 64) * 8
        + column // 128
    )

    def build(i, carry):
        row = lax.broadcasted_iota(jnp.int32, (64, 1024), 0) + i * 64
        here = pl.ds(pl.multiple_of(i * 64, 64), 64)
        perm[here, :] = jnp.where(row == by_owner, 1.0, 0.0).astype(BF16)
        final[here, :] = jnp.where(row == by_head, 1.0, 0.0).astype(BF16)
        return carry

    lax.fori_loop(0, 16, build, 0)

    def multiply(block, distances):
        side = xh if block == 0 else other
        total = acc[...]
        for d in distances:
            i = turn(z, d)
            total = total + jnp.dot(
                states[:, side, i].reshape(128, 256), weights[i, side].reshape(256, 512),
                preferred_element_type=F32,
            )
        acc[...] = total

    def chip_take(phase, hops):
        for hop in hops:
            for short in (0, 1):
                for sub in (0, 1):
                    if hop < 4 or not short:
                        k = w_index(phase, hop, short, sub)
                        half = c if short else 1 - c
                        slot = weights.at[turn(z, way * hop), xh if phase == 0 else other, half * 2 + sub]
                        remote(slot, slot, chip_send.at[k], chip_recv.at[k], twin).wait_recv()

    w_take(0, 1, 0)
    w_take(0, 1, 1)
    take_states()
    e_far.start()
    y_own(0)
    w_take(0, 2, 0)
    far_own(0)
    w_take(0, 2, 1)
    far_own(1)
    w_take(0, 3, 0)
    twin_own()
    y_relay(0)
    e_far_in.wait_recv()
    y_own(1)
    w_take(1, 1, 0)
    w_take(1, 1, 1)
    w_take(1, 2, 0)
    w_take(1, 2, 1)
    w_take(1, 3, 0)
    y_relay(1)
    w_take(0, 3, 1)
    w_take(0, 4, 0)
    w_take(1, 3, 1)
    w_take(1, 4, 0)
    chip_take(0, (1, 2, 3, 4))
    y_rest(0)
    multiply(0, range(8))
    y_rest(1)
    chip_take(1, (1, 2))
    multiply(1, (0, 1, 2, 6, 7))
    len_load.wait()
    chip_take(1, (3, 4))
    multiply(1, (3, 4, 5))

    row = lax.broadcasted_iota(jnp.int32, (128, 512), 0)
    place = (row // 64) * 512 + z * 64 + lax.rem(row, 64)
    total = acc[...]
    kept = jnp.where(place < len_ref[0], total, jnp.zeros_like(total)).astype(BF16).reshape(2, 2, 32, 512)
    sorted_parts = jnp.dot(
        kept[:, 0].reshape(64, 512), perm[pl.ds(0, 512), :], preferred_element_type=F32
    ) + jnp.dot(kept[:, 1].reshape(64, 512), perm[pl.ds(512, 512), :], preferred_element_type=F32)
    sorted_parts = sorted_parts.astype(BF16)
    for b in (0, 1):
        for j in range(RING):
            parts[b * RING + j] = sorted_parts[b * 32 : b * 32 + 32, j * 128 : j * 128 + 128]

    e_far.wait_send()
    for sub in (0, 1):
        w_far[sub].wait_send()

    def sent(to, carry):
        @pl.when(to != z)
        def _():
            slot = states.at[y, xh, z]
            remote(slot, slot, e_send.at[to], e_recv.at[to], {"z": z}).wait_send()

        return carry

    lax.fori_loop(0, RING, sent, 0)
    for block in (0, 1):
        for side in (0, 1):
            for distance in range(1, REACH[block][side] + 1):
                y_copy(block, side, 0, distance).wait_send()

    me = xh * RING + y

    for across in (1, 0):
        for dy in (4, 3, 5, 2, 6, 1, 7, 0):
            if across or dy:
                to_xh, to_y = (other if across else xh), turn(y, dy)
                remote(
                    parts.at[to_xh * RING + to_y], arrived.at[me], far_send.at[3], far_recv.at[3],
                    {"xh": to_xh, "y": to_y},
                ).start()
    arrived[me] = parts[me]
    for phase in (0, 1):
        for k in range(phase * 14, phase * 14 + 14):
            slot = weights.at[z, xh, 0]
            remote(slot, slot, z_send.at[k], z_recv.at[k], ahead).wait_send()
            remote(slot, slot, chip_send.at[k], chip_recv.at[k], twin).wait_send()
    for k in (28, 29):
        slot = weights.at[z, xh, 0]
        remote(slot, slot, chip_send.at[k], chip_recv.at[k], twin).wait_send()
    most = arrived.at[pl.ds(0, 2 * RING - 1)]
    last = remote(most, most, far_send.at[3], far_recv.at[3], mate)
    last.wait_recv()
    rows = [
        jnp.concatenate(
            [arrived[s * RING + j][:, p * 64 : p * 64 + 64] for j in range(RING) for s in (0, 1)], axis=1
        )
        for p in (0, 1)
    ]
    out_ref[...] = jnp.dot(jnp.concatenate(rows, axis=0), final[...], preferred_element_type=F32).reshape(64, 8, 128).astype(BF16)
    last.wait_send()


def local(encoded, lengths, kv_weight):
    states = encoded.reshape(2, 8, 4, 16, 256)
    vmem = pl.BlockSpec(memory_space=pltpu.VMEM)
    hbm = pl.BlockSpec(memory_space=pltpu.HBM)
    keys_values = pl.pallas_call(
        project,
        out_shape=pltpu.VMEM((64, 8, 128), BF16),
        in_specs=[hbm, hbm, hbm],
        out_specs=vmem,
        scratch_shapes=[
            pltpu.SMEM((1,), jnp.int32),
            pltpu.VMEM((2, 8, 4, 16, 256), BF16),
            pltpu.VMEM((256, 8, 128), BF16),
            pltpu.VMEM((256, 1024), BF16),
            pltpu.VMEM((8, 2, 8, 16, 256), BF16),
            pltpu.VMEM((8, 2, 4, 64, 512), BF16),
            pltpu.VMEM((128, 512), F32),
            pltpu.VMEM((1024, 1024), BF16),
            pltpu.VMEM((1024, 1024), BF16),
            pltpu.VMEM((16, 32, 128), BF16),
            pltpu.VMEM((16, 32, 128), BF16),
            pltpu.SemaphoreType.DMA((6,)),
            pltpu.SemaphoreType.DMA((4,)),
            pltpu.SemaphoreType.DMA((4,)),
            pltpu.SemaphoreType.DMA((8,)),
            pltpu.SemaphoreType.DMA((8,)),
            pltpu.SemaphoreType.DMA((16,)),
            pltpu.SemaphoreType.DMA((16,)),
            pltpu.SemaphoreType.DMA((28,)),
            pltpu.SemaphoreType.DMA((28,)),
            pltpu.SemaphoreType.DMA((30,)),
            pltpu.SemaphoreType.DMA((30,)),
        ],
        compiler_params=pltpu.CompilerParams(collective_id=0, has_side_effects=True),
        name="project",
    )(states, lengths, kv_weight)
    return keys_values.reshape(1, 64, 8, 128)


def solution(mesh):
    torus = Mesh(mesh.devices.reshape(4, 2, 2, 8, 8), ("xl", "c", "xh", "z", "y"))
    placed = (P(("xl", "c"), None, ("xh", "z")), P(("xl", "c")), P(("xh", "z"), "y", None))
    return jax.shard_map(
        local, mesh=torus, in_specs=placed, out_specs=P(("xl", "c"), ("xh", "z"), "y", None), check_vma=False
    )
```
